32 devices in a mesh: face: 8 (over z, core), sub: 4 (over y, x).
Axes of the slice: x: 2, y: 2, z: 4, core: 2. Of those that a mesh axis runs over, the one named last changes fastest.
Arguments:
- mesh_latent: bfloat16 [8192, 512], P(('face', 'sub')), may hold values from -6 to 6
- edge_latent: bfloat16 [65536, 512], P(('face', 'sub')), may hold values from -6 to 6
- grid_features: bfloat16 [8192, 384], P(('face', 'sub')), may hold values from -6 to 6
- senders: int32 [65536], P(('face', 'sub')), may hold values from 0 to 383, as said below
- receivers: int32 [65536], P(('face', 'sub')), may hold values from 0 to 255
- send_lists: int32 [32, 4, 32], P(('face', 'sub')), may hold values from -1 to 255, as said below
- link_sources: int32 [16384], P(('face', 'sub')), may hold values from 0 to 255
- link_targets: int32 [16384], P(('face', 'sub')), may hold values from 0 to 255
- node_area: float32 [8192], P(('face', 'sub')), may hold values from 0.25 to 4.5
- grid_weight: bfloat16 [384, 512], P(None, 'sub'), may hold values from -0.3125 to 0.3125
- encode_weight: bfloat16 [1024, 512], P('sub'), may hold values from -0.1875 to 0.1875
- edge_first: bfloat16 [1, 1536, 512], P(None, 'sub'), may hold values from -0.15625 to 0.15625
- edge_second: bfloat16 [1, 512, 512], P(None, 'sub'), may hold values from -0.25 to 0.25
- node_first: bfloat16 [1, 1024, 512], P(None, 'sub'), may hold values from -0.1875 to 0.1875
- node_second: bfloat16 [1, 512, 512], P(None, 'sub'), may hold values from -0.25 to 0.25
Outputs:
- mesh_result: bfloat16 [8192, 512], P(('face', 'sub'))
- edge_result: bfloat16 [65536, 512], P(('face', 'sub'))
- masses: float32 [1, 512], replicated
The draws below stay inside these ranges and needn't reach their ends.
Inputs may be any that keep to these rules, and one draw needn't show every extreme that they name: `send_lists`: entries are the sending partition's own node numbers, or -1 for an unused slot; in every list the used slots come first, hold distinct nodes and number 32 // 2 or more; for every list number some partition uses all 32 slots. `senders`: A value below 256 names one of the partition's own nodes; 256 + d * 32 + k names slot k of the list with number d that the partition receives, and that slot is always a used one.
All inputs are finite; a program needn't handle non-finite values.
Results may differ from the reference program's by a relative error of at most 0.008.
Values may be sent and summed in bfloat16 or wider, within the bound.
A program may use at most 64 MiB of HBM per device.

```python
import jax
import jax.numpy as jnp
from jax import lax

D = 512
GFEAT = 384
NODE_DEV = 256
EDGE_DEV = 2048
GRID_DEV = 256
LINK_DEV = 512
HALO = 32
LAYERS = 1
NODES = 8192
EDGES = 65536
GRIDS = 8192
LINKS = 16384
N_FACE = 8
N_SUB = 4


def halo_live(key):
    partitions = N_FACE * N_SUB
    first_key, second_key = jax.random.split(jax.random.fold_in(key, 11))
    live_count = jax.random.randint(first_key, (partitions, 4), HALO // 2, HALO + 1)
    full_device = jax.random.randint(second_key, (4,), 0, partitions)
    live_count = jnp.where(jnp.arange(partitions)[:, None] == full_device[None, :], HALO, live_count)
    return live_count.astype(jnp.int32)


def draw_send_lists(key, part):
    partitions = N_FACE * N_SUB
    live_count = halo_live(key)
    scores = jax.random.randint(jax.random.fold_in(key, 12), (partitions, 4, NODE_DEV), 0, 1 << 20)
    scores = scores * NODE_DEV + jnp.arange(NODE_DEV, dtype=jnp.int32)[None, None, :]
    ranking = jnp.argsort(scores, axis=-1).astype(jnp.int32)[:, :, :HALO]
    slot_index = jnp.arange(HALO, dtype=jnp.int32)
    return jnp.where(slot_index[None, None, :] < live_count[:, :, None], ranking, -1).astype(jnp.int32)


def draw_senders(key, part):
    partitions = N_FACE * N_SUB
    live_count = halo_live(key)
    first_key, second_key, third_key, fourth_key = jax.random.split(jax.random.fold_in(key, 13), 4)
    total = partitions * EDGE_DEV
    device_of = jnp.arange(total, dtype=jnp.int32) // EDGE_DEV
    face_index = device_of // N_SUB
    sub_index = device_of % N_SUB
    direction = jax.random.randint(first_key, (total,), 0, 4)
    source = jnp.where(direction == 0, (face_index - 1) % N_FACE * N_SUB + sub_index, jnp.where(direction == 1, (face_index + 1) % N_FACE * N_SUB + sub_index, jnp.where(direction == 2, face_index * N_SUB + (sub_index - 1) % N_SUB, face_index * N_SUB + (sub_index + 1) % N_SUB)))
    live_here = live_count[source, direction]
    slot_index = jax.random.randint(second_key, (total,), 0, 1 << 20) % live_here
    remote = NODE_DEV + direction * HALO + slot_index
    local_node = jax.random.randint(third_key, (total,), 0, NODE_DEV)
    use_halo = jax.random.randint(fourth_key, (total,), 0, 4) == 0
    return jnp.where(use_halo, remote, local_node).astype(jnp.int32)


def draw_node_area(key, part):
    ramp_scale = 1.0 + 2.0 * jnp.arange(NODES, dtype=jnp.float32) / NODES
    factor = jax.random.uniform(key, (NODES,), jnp.float32, 0.5, 1.5)
    return (ramp_scale * factor).astype(jnp.float32)


def place_ends(drawn, stream_key, low, high):
    index_at = [jax.random.randint(jax.random.fold_in(stream_key, axis), (), 0, length) for axis, length in enumerate(drawn.shape)]
    main_axis = drawn.shape.index(max(drawn.shape))
    neighbour = index_at[:main_axis] + [(index_at[main_axis] + 1) % drawn.shape[main_axis]] + index_at[main_axis + 1:]
    return drawn.at[tuple(index_at)].set(low).at[tuple(neighbour)].set(high)


def shard_levels(key, extent, cuts, smallest, largest):
    def one(axis_at, parts):
        draws = jax.random.uniform(jax.random.fold_in(jax.random.fold_in(key, 6), axis_at), (parts,), jnp.float32, smallest / len(cuts), largest / len(cuts))
        return jnp.repeat(jnp.exp(draws), extent[axis_at] // parts).reshape((-1,) + (1,) * (len(extent) - axis_at - 1))

    factor_of = one(*cuts[0])
    for cut in cuts[1:]:
        factor_of = factor_of * one(*cut)
    return factor_of


def centred(own_key, shape, deviation, limit, cuts=(), kind=jnp.bfloat16):
    gain = shard_levels(own_key, shape, cuts, -0.22, 0.18) if cuts else 1.0
    result = jax.random.normal(own_key, shape, jnp.float32) * deviation * gain
    return jnp.minimum(jnp.maximum(result, -limit), limit).astype(kind)


def setup_inputs(seed: int = 0) -> dict:
    key_of = jax.random.split(jax.random.key(seed), 16)
    return {
        "mesh_latent": centred(key_of[0], (NODES, D), 1.0, 6.0, ((0, 32),)),
        "edge_latent": centred(key_of[1], (EDGES, D), 1.0, 6.0, ((0, 32),)),
        "grid_features": centred(key_of[2], (GRIDS, GFEAT), 1.0, 6.0, ((0, 32),)),
        "senders": draw_senders(jax.random.fold_in(key_of[15], 71), 0),
        "receivers": place_ends(jax.random.randint(key_of[4], (EDGES,), 0, NODE_DEV), jax.random.fold_in(key_of[4], 1), 0, NODE_DEV - 1).astype(jnp.int32),
        "send_lists": draw_send_lists(jax.random.fold_in(key_of[15], 71), 0),
        "link_sources": place_ends(jax.random.randint(key_of[6], (LINKS,), 0, GRID_DEV), jax.random.fold_in(key_of[6], 1), 0, GRID_DEV - 1).astype(jnp.int32),
        "link_targets": place_ends(jax.random.randint(key_of[7], (LINKS,), 0, NODE_DEV), jax.random.fold_in(key_of[7], 1), 0, NODE_DEV - 1).astype(jnp.int32),
        "node_area": draw_node_area(jax.random.fold_in(key_of[15], 71), 0),
        "grid_weight": centred(key_of[9], (GFEAT, D), GFEAT ** -0.5, 0.3125, ((1, 4),)),
        "encode_weight": centred(key_of[10], (2 * D, D), (2 * D) ** -0.5, 0.1875, ((0, 4),)),
        "edge_first": centred(key_of[11], (LAYERS, 3 * D, D), (3 * D) ** -0.5, 0.15625, ((1, 4),)),
        "edge_second": centred(key_of[12], (LAYERS, D, D), D ** -0.5, 0.25, ((1, 4),)),
        "node_first": centred(key_of[13], (LAYERS, 2 * D, D), (2 * D) ** -0.5, 0.1875, ((1, 4),)),
        "node_second": centred(key_of[14], (LAYERS, D, D), D ** -0.5, 0.25, ((1, 4),)),
    }


def global_slots(send_lists):
    partitions = N_FACE * N_SUB
    part_ids = jnp.arange(partitions, dtype=jnp.int32)
    face_index = part_ids // N_SUB
    sub_index = part_ids % N_SUB
    sources = jnp.stack([((face_index - 1) % N_FACE) * N_SUB + sub_index,
                         ((face_index + 1) % N_FACE) * N_SUB + sub_index,
                         face_index * N_SUB + (sub_index - 1) % N_SUB,
                         face_index * N_SUB + (sub_index + 1) % N_SUB], axis=1).astype(jnp.int32)
    incoming_lists = send_lists[sources, jnp.arange(4, dtype=jnp.int32)[None, :], :]
    remote = jnp.where(incoming_lists >= 0, sources[:, :, None] * NODE_DEV + incoming_lists, NODES)
    own_rows = part_ids[:, None] * NODE_DEV + jnp.arange(NODE_DEV, dtype=jnp.int32)[None, :]
    return jnp.concatenate([own_rows, remote.reshape(partitions, 4 * HALO).astype(jnp.int32)], axis=1).astype(jnp.int32)


def reference(mesh_latent, edge_latent, grid_features, senders, receivers, send_lists, link_sources, link_targets, node_area, grid_weight, encode_weight, edge_first, edge_second, node_first, node_second):
    partitions = N_FACE * N_SUB
    grid_latent = jax.nn.silu(jnp.dot(grid_features, grid_weight, preferred_element_type=jnp.float32)).astype(jnp.bfloat16)

    def encode_block(block):
        grid_rows, node_rows, sources, targets = block
        joined = jnp.concatenate([jnp.take(grid_rows, sources, axis=0), jnp.take(node_rows, targets, axis=0)], axis=1)
        messages = jax.nn.silu(jnp.dot(joined, encode_weight, preferred_element_type=jnp.float32)).astype(jnp.bfloat16)
        return jax.ops.segment_sum(messages.astype(jnp.float32), targets, num_segments=NODE_DEV)

    gathered = lax.map(encode_block, (grid_latent.reshape(partitions, GRID_DEV, D),
                                      mesh_latent.reshape(partitions, NODE_DEV, D),
                                      link_sources.reshape(partitions, LINK_DEV),
                                      link_targets.reshape(partitions, LINK_DEV)))
    latent = (mesh_latent.astype(jnp.float32) + gathered.reshape(NODES, D)).astype(jnp.bfloat16)

    slot_table = global_slots(send_lists)
    offsets = (jnp.arange(partitions, dtype=jnp.int32) * NODE_DEV)[:, None]
    local_receivers = receivers.reshape(partitions, EDGE_DEV)
    global_receivers = (local_receivers + offsets).astype(jnp.int32)
    edge_senders = senders.reshape(partitions, EDGE_DEV)
    edge_state = edge_latent.reshape(partitions, EDGE_DEV, D)
    totals = []
    for layer_index in range(LAYERS):
        padded = jnp.concatenate([latent, jnp.zeros((1, D), jnp.bfloat16)], axis=0)
        first_weight = edge_first[layer_index]
        second_weight = edge_second[layer_index]

        def edge_block(block):
            edges, slots, sends, global_recv, local_recv = block
            joined = jnp.concatenate([edges, jnp.take(padded, jnp.take(slots, sends), axis=0),
                                      jnp.take(latent, global_recv, axis=0)], axis=1)
            hidden = jax.nn.silu(jnp.dot(joined, first_weight, preferred_element_type=jnp.float32)).astype(jnp.bfloat16)
            updated = (edges.astype(jnp.float32) + jnp.dot(hidden, second_weight, preferred_element_type=jnp.float32)).astype(jnp.bfloat16)
            incoming = jax.ops.segment_sum(updated.astype(jnp.float32), local_recv, num_segments=NODE_DEV)
            return updated, incoming

        edge_state, incoming = lax.map(edge_block, (edge_state, slot_table, edge_senders, global_receivers, local_receivers))
        incoming = incoming.reshape(NODES, D).astype(jnp.bfloat16)
        node_hidden = jax.nn.silu(jnp.dot(jnp.concatenate([latent, incoming], axis=1), node_first[layer_index],
                                          preferred_element_type=jnp.float32)).astype(jnp.bfloat16)
        latent = (latent.astype(jnp.float32) + jnp.dot(node_hidden, node_second[layer_index],
                                                       preferred_element_type=jnp.float32)).astype(jnp.bfloat16)
        totals.append(jnp.dot(node_area, latent.astype(jnp.float32), precision=lax.Precision.HIGHEST))
    masses = jnp.stack(totals) / NODES
    return latent, edge_state.reshape(EDGES, D), masses
```

```python
import functools

import jax
import jax.numpy as jnp
from jax import lax
from jax.experimental import pallas as pl
from jax.experimental.pallas import tpu as pltpu
from jax.sharding import PartitionSpec as P

MESH = pl.DeviceIdType.MESH
CHUNK = 512
LANES = 128
QUARTERED = (1, 2)
BF = jnp.bfloat16
F32 = jnp.float32


def silu(v):
    return v / (1.0 + jnp.exp(-v))


def mm(a, b):
    return jnp.dot(a, b, preferred_element_type=F32)


def mm_t(a, b):
    return lax.dot_general(a, b, (((0,), (0,)), ((), ())), preferred_element_type=F32)


def hot(rows, index):
    ids = lax.broadcasted_iota(jnp.int32, (rows, index.shape[1]), 0)
    return jnp.where(ids == index, 1.0, 0.0).astype(BF)


def kernel(
    n_face, n_sub,
    mesh_hbm, edge_hbm, grid_hbm, send_hbm, recv_hbm, lists_hbm, src_hbm, dst_hbm, area_hbm,
    wg, we, w1, w2, v1, v2,
    lat_out, edges, mass_out,
    gg, ge, g1, g2, h1, h2,
    mesh_ref, grid_ref, send_ref, recv_ref, lists_ref, src_ref, dst_ref, area_ref,
    picks, back, table, proj, halo, parts, total, hiddens, area_col,
    s1, r1, s2, r2, s3, r3, hs, hr, ms, mr, ein, win, pin,
):
    face, sub = lax.axis_index("face"), lax.axis_index("sub")
    core = lax.rem(face, 2)
    partner = face + 1 - 2 * core
    level = lax.rem(face // 2, 2)
    beside = face + 2 - 4 * level
    nodes, width = mesh_ref.shape
    chunks = edges.shape[0] // CHUNK

    def load_edges(i):
        rows = pl.ds(pl.multiple_of(i * CHUNK, CHUNK), CHUNK)
        return pltpu.make_async_copy(edge_hbm.at[rows], edges.at[rows], ein.at[i])

    shards = [wg, we, w1.at[0], w2.at[0], v1.at[0], v2.at[0]]
    wholes = [gg, ge, g1, g2, h1, h2]

    def own(w):
        rows = shards[w].shape[0]
        slot = gg.at[sub] if w == 0 else wholes[w].at[pl.ds(pl.multiple_of(sub * rows, rows), rows)]
        return pltpu.make_async_copy(shards[w], slot, win.at[w])

    pairs = [(send_hbm, send_ref), (recv_hbm, recv_ref), (src_hbm, src_ref), (dst_hbm, dst_ref),
             (grid_hbm, grid_ref), (mesh_hbm, mesh_ref), (lists_hbm, lists_ref), (area_hbm, area_ref)]
    loads = [pltpu.make_async_copy(a, b, pin.at[i]) for i, (a, b) in enumerate(pairs)]
    for w in range(6):
        own(w).start()
    for copy in loads:
        copy.start()
    for i in range(chunks):
        load_edges(i).start()

    others = [(lax.rem(face + a, n_face), lax.rem(sub + b, n_sub))
              for a in range(n_face) for b in range(n_sub) if a or b]
    barrier = pltpu.get_barrier_semaphore()
    for peer in others:
        pl.semaphore_signal(barrier, inc=1, device_id=peer, device_id_type=MESH)
    pl.semaphore_wait(barrier, len(others))

    def half_of(w, owner):
        rows = shards[w].shape[0]
        half = rows // 2
        if w == 0:
            return gg.at[owner, pl.ds(pl.multiple_of(core * half, half), half)]
        return wholes[w].at[pl.ds(pl.multiple_of(owner * rows + core * half, half), half)]

    def quarter_of(w, owner):
        rows = shards[w].shape[0]
        piece = rows // 4
        start = (core * 2 + level) * piece
        if w == 0:
            return gg.at[owner, pl.ds(pl.multiple_of(start, piece), piece)]
        return wholes[w].at[pl.ds(pl.multiple_of(owner * rows + start, piece), piece)]

    def outward(w, k):
        part = quarter_of(w, sub) if w in QUARTERED else half_of(w, sub)
        return pltpu.make_async_remote_copy(
            src_ref=part, dst_ref=part,
            send_sem=s1.at[w, k], recv_sem=r1.at[w, k],
            device_id=(face, lax.rem(sub + k, n_sub)), device_id_type=MESH)

    def upward(w, k):
        part = quarter_of(w, lax.rem(sub + n_sub - k, n_sub))
        return pltpu.make_async_remote_copy(
            src_ref=part, dst_ref=part, send_sem=s3.at[w, k], recv_sem=r3.at[w, k],
            device_id=(beside, sub), device_id_type=MESH)

    def across(w, k):
        part = half_of(w, lax.rem(sub + n_sub - k, n_sub))
        return pltpu.make_async_remote_copy(
            src_ref=part, dst_ref=part, send_sem=s2.at[w, k], recv_sem=r2.at[w, k],
            device_id=(partner, sub), device_id_type=MESH)

    def send(w):
        own(w).wait()
        for k in range(1, n_sub):
            outward(w, k).start()

    for w in range(4):
        send(w)
    for copy in loads:
        copy.wait()

    def climb(w):
        for k in range(1, n_sub):
            if w in QUARTERED:
                outward(w, k).wait_recv()
                upward(w, k).start()

    def pass_on(w):
        for k in range(1, n_sub):
            if w in QUARTERED:
                upward(w, k).wait_recv()
            else:
                outward(w, k).wait_recv()
            across(w, k).start()

    def arrive(w):
        for k in range(1, n_sub):
            across(w, k).wait_recv()

    slots = nodes + 4 * halo.shape[1]

    def mark(i, carry):
        cols = pl.ds(pl.multiple_of(i * CHUNK, CHUNK), CHUNK)
        here = hot(nodes, recv_ref[:, cols])
        back[:, cols] = here
        both = jnp.concatenate([hot(slots, send_ref[:, cols]), here], axis=0)
        picks[cols, :] = both.T
        return carry

    lax.fori_loop(0, chunks, mark, 0)
    for i in range(chunks):
        load_edges(i).wait()
    total[...] = jnp.zeros_like(total)

    def collect(i, carry):
        cols = pl.ds(pl.multiple_of(i * CHUNK, CHUNK), CHUNK)
        total[...] += mm(back[:, cols], edges[cols, :])
        return carry

    lax.fori_loop(0, chunks, collect, 0)
    area_col[...] = jnp.broadcast_to(area_ref[...], (LANES, nodes)).T
    to_node = hot(nodes, dst_ref[...])
    link_pick = jnp.concatenate([hot(grid_ref.shape[0], src_ref[...]), to_node], axis=0)

    pass_on(0)
    climb(1)
    arrive(0)
    grid = jnp.concatenate([mm(grid_ref[...], gg[j]) for j in range(n_sub)], axis=1)
    grid = silu(grid).astype(BF)
    pass_on(1)
    climb(2)
    arrive(1)
    rows = grid_ref.shape[0]
    from_grid = mm(grid, ge[:width, :]).astype(BF)
    from_mesh = mm(mesh_ref[...], ge[width:, :]).astype(BF)
    message = silu(mm_t(link_pick, jnp.concatenate([from_grid, from_mesh], axis=0))).astype(BF)
    latent = (mesh_ref[...].astype(F32) + mm(to_node, message)).astype(BF)
    table[...] = latent

    size = halo.shape[1]
    for d in range(4):
        halo[d] = mm_t(hot(nodes, lists_ref[0, d:d + 1, :]), latent).astype(BF)

    def border(d):
        step = (1, n_face - 1, 1, n_sub - 1)[d]
        to = (lax.rem(face + step, n_face), sub) if d < 2 else (face, lax.rem(sub + step, n_sub))
        return pltpu.make_async_remote_copy(
            src_ref=halo.at[d], dst_ref=halo.at[4 + d], send_sem=hs.at[d], recv_sem=hr.at[d],
            device_id=to, device_id_type=MESH)

    for d in range(4):
        border(d).start()
    send(4)
    send(5)

    pass_on(2)
    arrive(2)
    proj[:nodes, :] = mm(latent, g1[width:2 * width, :]).astype(BF)
    proj[slots:, :] = mm(latent, g1[2 * width:, :]).astype(BF)
    for d in range(4):
        border(d).wait_recv()
    outer = jnp.concatenate([halo[4 + d] for d in range(4)], axis=0)
    proj[nodes:slots, :] = mm(outer, g1[width:2 * width, :]).astype(BF)
    pass_on(3)
    arrive(3)

    into = jnp.zeros((nodes, width), F32)

    def first(i, into):
        cols = pl.ds(pl.multiple_of(i * CHUNK, CHUNK), CHUNK)
        before = mm(edges[cols, :], g1[:width, :]) + mm(picks[cols, :], proj[...])
        hidden = silu(before).astype(BF)
        hiddens[cols, :] = hidden
        return into + mm(back[:, cols], hidden)

    into = lax.fori_loop(0, chunks // 2, first, into)
    climb(4)
    into = lax.fori_loop(chunks // 2, chunks, first, into)
    pass_on(4)
    pass_on(5)
    high = into.astype(BF)
    low = (into - high.astype(F32)).astype(BF)
    incoming = (total[...] + (mm(high, g2[...]) + mm(low, g2[...]))).astype(BF)
    arrive(4)
    hidden = silu(mm(table[...], h1[:width, :]) + mm(incoming, h1[width:, :])).astype(BF)
    arrive(5)
    final = (table[...].astype(F32) + mm(hidden, h2[...])).astype(BF)
    lat_out[...] = final
    weight = jnp.concatenate([area_col[...]] * (width // LANES), axis=1)
    me = face * n_sub + sub
    parts[me] = jnp.sum(final.astype(F32) * weight, axis=0, keepdims=True)

    def share(k):
        return pltpu.make_async_remote_copy(
            src_ref=parts.at[me], dst_ref=parts.at[me], send_sem=ms.at[k], recv_sem=mr.at[k],
            device_id=others[k], device_id_type=MESH)

    for k in range(len(others)):
        share(k).start()

    def second(i, carry):
        cols = pl.ds(pl.multiple_of(i * CHUNK, CHUNK), CHUNK)
        edges[cols, :] = (edges[cols, :].astype(F32) + mm(hiddens[cols, :], g2[...])).astype(BF)
        return carry

    lax.fori_loop(0, chunks, second, 0)
    for k in range(len(others)):
        share(k).wait_recv()
    mass_out[...] = jnp.sum(parts[...], axis=0) / (nodes * n_face * n_sub)

    for w in range(6):
        for k in range(1, n_sub):
            outward(w, k).wait_send()
            across(w, k).wait_send()
            if w in QUARTERED:
                upward(w, k).wait_send()
    for d in range(4):
        border(d).wait_send()
    for k in range(len(others)):
        share(k).wait_send()


def put(lat, edges, mass, lat_out, edges_out, mass_out, sems):
    pairs = [(edges, edges_out), (lat, lat_out), (mass, mass_out)]
    copies = [pltpu.make_async_copy(a, b, sems.at[i]) for i, (a, b) in enumerate(pairs)]
    for copy in copies:
        copy.start()
    for copy in copies:
        copy.wait()


def per_device(
    mesh_latent, edge_latent, grid_features, senders, receivers, send_lists, link_sources,
    link_targets, node_area, grid_weight, encode_weight, edge_first, edge_second, node_first,
    node_second,
):
    n_face, n_sub = lax.axis_size("face"), lax.axis_size("sub")
    nodes, width = mesh_latent.shape
    count = edge_latent.shape[0]
    size = send_lists.shape[2]
    slots = nodes + 4 * size
    chunks = count // CHUNK
    dma = pltpu.SemaphoreType.DMA
    vmem = pl.BlockSpec(memory_space=pltpu.VMEM)
    hbm = pl.BlockSpec(memory_space=pltpu.HBM)
    anywhere = pl.BlockSpec(memory_space=pl.ANY)
    whole = [pltpu.VMEM((n_sub * w.shape[-2], width), BF)
             for w in (encode_weight, edge_first, edge_second, node_first, node_second)]
    results = pl.pallas_call(
        functools.partial(kernel, n_face, n_sub),
        out_shape=(
            pltpu.VMEM(mesh_latent.shape, BF),
            pltpu.VMEM(edge_latent.shape, BF),
            pltpu.VMEM((1, width), F32),
        ),
        in_specs=[hbm] * 15,
        out_specs=(vmem, vmem, vmem),
        scratch_shapes=[
            pltpu.VMEM((n_sub,) + grid_weight.shape, BF), *whole,
            pltpu.VMEM(mesh_latent.shape, BF), pltpu.VMEM(grid_features.shape, BF),
            pltpu.VMEM((1, count), jnp.int32), pltpu.VMEM((1, count), jnp.int32),
            pltpu.VMEM(send_lists.shape, jnp.int32),
            pltpu.VMEM((1, link_sources.shape[0]), jnp.int32),
            pltpu.VMEM((1, link_targets.shape[0]), jnp.int32),
            pltpu.VMEM((1, nodes), F32),
            pltpu.VMEM((count, slots + nodes), BF),
            pltpu.VMEM((nodes, count), BF),
            pltpu.VMEM((nodes, width), BF),
            pltpu.VMEM((slots + nodes, width), BF),
            pltpu.VMEM((8, size, width), BF),
            pltpu.VMEM((n_face * n_sub, 1, width), F32),
            pltpu.VMEM((nodes, width), F32),
            pltpu.VMEM(edge_latent.shape, BF),
            pltpu.VMEM((nodes, LANES), F32),
            *[dma((6, n_sub))] * 6,
            dma((4,)), dma((4,)), dma((n_face * n_sub,)), dma((n_face * n_sub,)),
            dma((chunks,)), dma((6,)), dma((8,)),
        ],
        compiler_params=pltpu.CompilerParams(
            collective_id=0, has_side_effects=True, vmem_limit_bytes=62000000
        ),
    )(
        mesh_latent, edge_latent, grid_features, senders.reshape(1, -1), receivers.reshape(1, -1),
        send_lists, link_sources.reshape(1, -1), link_targets.reshape(1, -1),
        node_area.reshape(1, -1), grid_weight, encode_weight, edge_first, edge_second, node_first,
        node_second,
    )
    return pl.pallas_call(
        put,
        out_shape=tuple(jax.ShapeDtypeStruct(r.shape, r.dtype) for r in results),
        in_specs=[anywhere] * 3,
        out_specs=(anywhere,) * 3,
        scratch_shapes=[dma((3,))],
        compiler_params=pltpu.CompilerParams(vmem_limit_bytes=1 << 20),
    )(*results)


def solution(mesh):
    both = P(("face", "sub"))
    in_specs = (both,) * 9 + (P(None, "sub"), P("sub", None)) + (P(None, "sub", None),) * 4
    return jax.shard_map(
        per_device, mesh=mesh, in_specs=in_specs, out_specs=(both, both, P()), check_vma=False
    )
```

```python
import functools

import jax
import jax.numpy as jnp
from jax import lax
from jax.experimental import pallas as pl
from jax.experimental.pallas import tpu as pltpu
from jax.sharding import PartitionSpec as P

MESH = pl.DeviceIdType.MESH
CHUNK = 512
LANES = 128
LEVELLED = (1, 4)
BF = jnp.bfloat16
F32 = jnp.float32


def silu(v):
    return v / (1.0 + jnp.exp(-v))


def mm(a, b):
    return jnp.dot(a, b, preferred_element_type=F32)


def mm_t(a, b):
    return lax.dot_general(a, b, (((0,), (0,)), ((), ())), preferred_element_type=F32)


def hot(rows, index):
    ids = lax.broadcasted_iota(jnp.int32, (rows, index.shape[1]), 0)
    return jnp.where(ids == index, 1.0, 0.0).astype(BF)


PLAN = (
    ("first", 1), ("first", 0), ("second", 0), ("second", 1), ("first", 4), ("turn", 1), ("turn", 0),
    ("first", 2), ("direct", 1), ("last", 1), ("turn", 4), ("last", 0), ("second", 2), ("links", None),
    ("direct", 0), ("lift1", 1), ("mark", None), ("turn", 2), ("collect", None), ("lift2", 1), ("first", 5),
    ("lift3", 1), ("second", 4), ("first", 3), ("last", 4), ("arrive", 0), ("embed", None), ("second", 3),
    ("lift1", 4), ("arrive", 1), ("encode", None), ("ring", None), ("second", 5), ("direct", 2), ("last", 2),
    ("direct", 4), ("turn", 5), ("arrive", 2), ("turn", 3), ("project", None), ("direct", 3), ("hide0", None),
    ("direct", 5), ("lift2", 4), ("last", 5), ("last", 3), ("lift3", 4), ("hide1", None), ("arrive", 3),
    ("gather", None),
)


def kernel(
    n_face, n_sub,
    mesh_hbm, edge_hbm, grid_hbm, send_hbm, recv_hbm, lists_hbm, src_hbm, dst_hbm, area_hbm,
    wg, we, w1, w2, v1, v2,
    lat_out, edges, mass_out,
    gg, ge, g1, g2, h1, h2,
    mesh_ref, grid_ref, send_ref, recv_ref, lists_ref, src_ref, dst_ref, area_ref,
    picks, back, link_pick, table, proj, halo, parts, total, into, hiddens, area_col,
    s1, r1, s2, r2, s3, r3, hs, hr, ms, mr, ein, win, pin,
):
    face, sub = lax.axis_index("face"), lax.axis_index("sub")
    core = lax.rem(face, 2)
    partner = face + 1 - 2 * core
    level = lax.rem(face // 2, 2)
    beside = face + 2 - 4 * level
    nodes, width = mesh_ref.shape
    chunks = edges.shape[0] // CHUNK
    size = halo.shape[1]
    slots = nodes + 4 * size

    load_edges = pltpu.make_async_copy(edge_hbm, edges, ein)

    shards = [wg, we, w1.at[0], w2.at[0], v1.at[0], v2.at[0]]
    wholes = [gg, ge, g1, g2, h1, h2]

    def rows_of(w, owner, start, count):
        rows = shards[w].shape[0]
        return wholes[w].at[pl.ds(pl.multiple_of(owner * rows + start, count), count)]

    def own(w):
        return pltpu.make_async_copy(shards[w], rows_of(w, sub, 0, shards[w].shape[0]), win.at[w])

    pairs = [(send_hbm, send_ref), (recv_hbm, recv_ref), (src_hbm, src_ref), (dst_hbm, dst_ref),
             (grid_hbm, grid_ref), (mesh_hbm, mesh_ref), (lists_hbm, lists_ref), (area_hbm, area_ref)]
    loads = [pltpu.make_async_copy(a, b, pin.at[i]) for i, (a, b) in enumerate(pairs)]
    for w in range(6):
        own(w).start()
    for copy in loads:
        copy.start()
    load_edges.start()

    others = [(lax.rem(face + a, n_face), lax.rem(sub + b, n_sub))
              for a in range(n_face) for b in range(n_sub) if a or b]
    barrier = pltpu.get_barrier_semaphore()
    for peer in others:
        pl.semaphore_signal(barrier, inc=1, device_id=peer, device_id_type=MESH)
    pl.semaphore_wait(barrier, len(others))

    bits = [1 << b for b in range(n_sub.bit_length() - 1)]
    orders = (bits, bits[::-1])
    masks = range(1, n_sub)

    def across_bits(mask):
        index = sub
        for bit in bits:
            if mask & bit:
                index = index + bit - 2 * bit * lax.rem(index // bit, 2)
        return index

    def top(path, mask):
        return max(t for t, bit in enumerate(orders[path]) if mask & bit)

    def piece(w, path, mask, other_level=False):
        rows = shards[w].shape[0]
        if w in LEVELLED:
            count = rows // 8
            at = 1 - level if other_level else level
            start = (core * 4 + at * 2 + path) * count
        else:
            count = rows // 4
            start = (core * 2 + path) * count
        return rows_of(w, across_bits(mask), start, count)

    final = len(bits) - 1
    groups = [[(p, m) for m in masks for p in (0, 1) if top(p, m) == t] for t in range(final)]
    groups.append([(p, m) for p in (0, 1) for m in bits if top(p, m) == final])
    groups.append([(p, m) for m in masks for p in (0, 1) if top(p, m) == final and m not in bits])
    turns, direct, last = range(final), (final,), (final + 1,)
    group_of = {pm: g for g, group in enumerate(groups) for pm in group}

    def settle(w, count, sem):
        rows = wholes[w].at[pl.ds(0, count)]
        pltpu.make_async_copy(rows, rows, sem).wait()

    def cut(w):
        return shards[w].shape[0] // (8 if w in LEVELLED else 4)

    def outward(w, path, mask):
        bit = orders[path][top(path, mask)]
        part = piece(w, path, mask - bit)
        return pltpu.make_async_remote_copy(
            src_ref=part, dst_ref=part, send_sem=s1.at[w], recv_sem=r1.at[w, group_of[path, mask]],
            device_id=(face, across_bits(bit)), device_id_type=MESH)

    def upward(w, path, mask):
        part = piece(w, path, mask)
        at = LEVELLED.index(w)
        return pltpu.make_async_remote_copy(
            src_ref=part, dst_ref=part, send_sem=s3.at[at], recv_sem=r3.at[at, group_of[path, mask]],
            device_id=(beside, sub), device_id_type=MESH)

    def across(w, path, mask, lifted):
        part = piece(w, path, mask, lifted)
        return pltpu.make_async_remote_copy(
            src_ref=part, dst_ref=part, send_sem=s2.at[w], recv_sem=r2.at[w],
            device_id=(partner, sub), device_id_type=MESH)

    def begin(w):
        own(w).wait()
        for p in (0, 1):
            outward(w, p, orders[p][0]).start()

    def rest(w):
        for p in (0, 1):
            for bit in orders[p][1:]:
                outward(w, p, bit).start()

    def take(which, w):
        for g in which:
            if not groups[g]:
                continue
            settle(w, len(groups[g]) * cut(w), r1.at[w, g])
            for p, m in groups[g]:
                for bit in orders[p][top(p, m) + 1:]:
                    outward(w, p, m + bit).start()
                if w in LEVELLED:
                    upward(w, p, m).start()
                across(w, p, m, False).start()

    def lift(which, w):
        for g in which:
            if not groups[g]:
                continue
            settle(w, len(groups[g]) * cut(w), r3.at[LEVELLED.index(w), g])
            for p, m in groups[g]:
                across(w, p, m, True).start()

    def arrive(w):
        settle(w, (n_sub - 1) * shards[w].shape[0] // 2, r2.at[w])

    def border(d):
        step = (1, n_face - 1, 1, n_sub - 1)[d]
        to = (lax.rem(face + step, n_face), sub) if d < 2 else (face, lax.rem(sub + step, n_sub))
        return pltpu.make_async_remote_copy(
            src_ref=halo.at[d], dst_ref=halo.at[4 + d], send_sem=hs, recv_sem=hr,
            device_id=to, device_id_type=MESH)

    def ready():
        while loads:
            loads.pop().wait()

    def mark():
        ready()

        def step(i, carry):
            cols = pl.ds(pl.multiple_of(i * CHUNK, CHUNK), CHUNK)
            here = hot(nodes, recv_ref[:, cols])
            back[:, cols] = here
            both = jnp.concatenate([hot(slots, send_ref[:, cols]), here], axis=0)
            picks[cols, :] = both.T
            return carry

        lax.fori_loop(0, chunks, step, 0)

    def collect():
        load_edges.wait()
        total[...] = mm(back[...], edges[...])
        into[...] = jnp.zeros_like(into)
        area_col[...] = jnp.broadcast_to(area_ref[...], (LANES, nodes)).T

    grids = grid_ref.shape[0]

    def links():
        ready()
        link_pick[:grids, :] = hot(grids, src_ref[...])
        link_pick[grids:, :] = hot(nodes, dst_ref[...])

    def embed():
        depth = grid_ref.shape[1]
        grid = jnp.concatenate([mm(grid_ref[...], gg[j * depth:(j + 1) * depth, :]) for j in range(n_sub)], axis=1)
        table[...] = silu(grid).astype(BF)

    def encode():
        from_grid = mm(table[...], ge[:width, :]).astype(BF)
        from_mesh = mm(mesh_ref[...], ge[width:, :]).astype(BF)
        both = jnp.concatenate([from_grid, from_mesh], axis=0)
        message = silu(mm_t(link_pick[...], both)).astype(BF)
        table[...] = (mesh_ref[...].astype(F32) + mm(link_pick[grids:, :], message)).astype(BF)

    def ring():
        for d in range(4):
            halo[d] = mm_t(hot(nodes, lists_ref[0, d:d + 1, :]), table[...]).astype(BF)
        for d in range(4):
            border(d).start()

    def project():
        proj[:nodes, :] = mm(table[...], g1[width:2 * width, :]).astype(BF)
        proj[slots:, :] = mm(table[...], g1[2 * width:, :]).astype(BF)
        lists = halo.at[pl.ds(0, 4)]
        pltpu.make_async_copy(lists, lists, hr).wait()
        outer = jnp.concatenate([halo[4 + d] for d in range(4)], axis=0)
        proj[nodes:slots, :] = mm(outer, g1[width:2 * width, :]).astype(BF)

    def hide(part):
        def step(i, carry):
            cols = pl.ds(pl.multiple_of(i * CHUNK, CHUNK), CHUNK)
            before = mm(edges[cols, :], g1[:width, :]) + mm(picks[cols, :], proj[...])
            hidden = silu(before).astype(BF)
            hiddens[cols, :] = hidden
            into[...] += mm(back[:, cols], hidden)
            return carry

        lax.fori_loop(part * chunks // 2, (part + 1) * chunks // 2, step, 0)

    def gather():
        high = into[...].astype(BF)
        low = (into[...] - high.astype(F32)).astype(BF)
        total[...] += mm(high, g2[...]) + mm(low, g2[...])

    steps = {
        "first": begin, "second": rest, "arrive": arrive,
        "turn": functools.partial(take, turns), "direct": functools.partial(take, direct),
        "last": functools.partial(take, last), "lift1": functools.partial(lift, turns),
        "lift2": functools.partial(lift, direct), "lift3": functools.partial(lift, last),
    }
    works = {"mark": mark, "collect": collect, "links": links, "embed": embed, "encode": encode, "ring": ring,
             "project": project, "hide0": functools.partial(hide, 0), "hide1": functools.partial(hide, 1),
             "gather": gather}
    for name, w in PLAN:
        if w is None:
            works[name]()
        else:
            steps[name](w)

    arrive(4)
    incoming = total[...].astype(BF)
    hidden = silu(mm(table[...], h1[:width, :]) + mm(incoming, h1[width:, :])).astype(BF)
    arrive(5)
    latest = (table[...].astype(F32) + mm(hidden, h2[...])).astype(BF)
    lat_out[...] = latest
    weight = jnp.concatenate([area_col[...]] * (width // LANES), axis=1)
    me = face * n_sub + sub
    parts[me] = jnp.sum(latest.astype(F32) * weight, axis=0, keepdims=True)

    def share(k):
        return pltpu.make_async_remote_copy(
            src_ref=parts.at[me], dst_ref=parts.at[me], send_sem=ms, recv_sem=mr,
            device_id=others[k], device_id_type=MESH)

    for k in range(len(others)):
        share(k).start()

    def update(i, carry):
        cols = pl.ds(pl.multiple_of(i * CHUNK, CHUNK), CHUNK)
        edges[cols, :] = (edges[cols, :].astype(F32) + mm(hiddens[cols, :], g2[...])).astype(BF)
        return carry

    lax.fori_loop(0, chunks, update, 0)
    heard = parts.at[pl.ds(0, len(others))]
    pltpu.make_async_copy(heard, heard, mr).wait()
    mass_out[...] = jnp.sum(parts[...], axis=0) / (nodes * n_face * n_sub)

    for w in range(6):
        settle(w, 2 * (n_sub - 1) * cut(w), s1.at[w])
        settle(w, (n_sub - 1) * shards[w].shape[0] // 2, s2.at[w])
        if w in LEVELLED:
            settle(w, 2 * (n_sub - 1) * cut(w), s3.at[LEVELLED.index(w)])
    pltpu.make_async_copy(halo.at[pl.ds(0, 4)], halo.at[pl.ds(0, 4)], hs).wait()
    pltpu.make_async_copy(heard, heard, ms).wait()


def put(lat, edges, mass, lat_out, edges_out, mass_out, sems):
    pairs = [(edges, edges_out), (lat, lat_out), (mass, mass_out)]
    copies = [pltpu.make_async_copy(a, b, sems.at[i]) for i, (a, b) in enumerate(pairs)]
    for copy in copies:
        copy.start()
    for copy in copies:
        copy.wait()


def per_device(
    mesh_latent, edge_latent, grid_features, senders, receivers, send_lists, link_sources,
    link_targets, node_area, grid_weight, encode_weight, edge_first, edge_second, node_first,
    node_second,
):
    n_face, n_sub = lax.axis_size("face"), lax.axis_size("sub")
    nodes, width = mesh_latent.shape
    count = edge_latent.shape[0]
    size = send_lists.shape[2]
    slots = nodes + 4 * size
    chunks = count // CHUNK
    dma = pltpu.SemaphoreType.DMA
    turns = n_sub.bit_length()
    vmem = pl.BlockSpec(memory_space=pltpu.VMEM)
    hbm = pl.BlockSpec(memory_space=pltpu.HBM)
    anywhere = pl.BlockSpec(memory_space=pl.ANY)
    whole = [pltpu.VMEM((n_sub * w.shape[-2], width), BF)
             for w in (encode_weight, edge_first, edge_second, node_first, node_second)]
    results = pl.pallas_call(
        functools.partial(kernel, n_face, n_sub),
        out_shape=(
            pltpu.VMEM(mesh_latent.shape, BF),
            pltpu.VMEM(edge_latent.shape, BF),
            pltpu.VMEM((1, width), F32),
        ),
        in_specs=[hbm] * 15,
        out_specs=(vmem, vmem, vmem),
        scratch_shapes=[
            pltpu.VMEM((n_sub * grid_weight.shape[0], grid_weight.shape[1]), BF), *whole,
            pltpu.VMEM(mesh_latent.shape, BF), pltpu.VMEM(grid_features.shape, BF),
            pltpu.VMEM((1, count), jnp.int32), pltpu.VMEM((1, count), jnp.int32),
            pltpu.VMEM(send_lists.shape, jnp.int32),
            pltpu.VMEM((1, link_sources.shape[0]), jnp.int32),
            pltpu.VMEM((1, link_targets.shape[0]), jnp.int32),
            pltpu.VMEM((1, nodes), F32),
            pltpu.VMEM((count, slots + nodes), BF),
            pltpu.VMEM((nodes, count), BF),
            pltpu.VMEM((grid_features.shape[0] + nodes, link_sources.shape[0]), BF),
            pltpu.VMEM((nodes, width), BF),
            pltpu.VMEM((slots + nodes, width), BF),
            pltpu.VMEM((8, size, width), BF),
            pltpu.VMEM((n_face * n_sub, 1, width), F32),
            pltpu.VMEM((nodes, width), F32),
            pltpu.VMEM((nodes, width), F32),
            pltpu.VMEM(edge_latent.shape, BF),
            pltpu.VMEM((nodes, LANES), F32),
            dma((6,)), dma((6, turns)), dma((6,)), dma((6,)), dma((len(LEVELLED),)), dma((len(LEVELLED), turns)),
            *[dma(())] * 5, dma((6,)), dma((8,)),
        ],
        compiler_params=pltpu.CompilerParams(
            collective_id=0, has_side_effects=True, vmem_limit_bytes=62000000
        ),
    )(
        mesh_latent, edge_latent, grid_features, senders.reshape(1, -1), receivers.reshape(1, -1),
        send_lists, link_sources.reshape(1, -1), link_targets.reshape(1, -1),
        node_area.reshape(1, -1), grid_weight, encode_weight, edge_first, edge_second, node_first,
        node_second,
    )
    return pl.pallas_call(
        put,
        out_shape=tuple(jax.ShapeDtypeStruct(r.shape, r.dtype) for r in results),
        in_specs=[anywhere] * 3,
        out_specs=(anywhere,) * 3,
        scratch_shapes=[dma((3,))],
        compiler_params=pltpu.CompilerParams(vmem_limit_bytes=1 << 20),
    )(*results)


def solution(mesh):
    both = P(("face", "sub"))
    in_specs = (both,) * 9 + (P(None, "sub"), P("sub", None)) + (P(None, "sub", None),) * 4
    return jax.shard_map(
        per_device, mesh=mesh, in_specs=in_specs, out_specs=(both, both, P()), check_vma=False
    )
```

```python
import functools

import jax
import jax.numpy as jnp
from jax import lax
from jax.experimental import pallas as pl
from jax.experimental.pallas import tpu as pltpu
from jax.sharding import PartitionSpec as P

MESH = pl.DeviceIdType.MESH
CHUNK = 1024
LANES = 128
LEVELLED = (1, 4)
BF = jnp.bfloat16
F32 = jnp.float32


def silu(v):
    return v / (1.0 + jnp.exp(-v))


def mm(a, b):
    return jnp.dot(a, b, preferred_element_type=F32)


def mm_t(a, b):
    return lax.dot_general(a, b, (((0,), (0,)), ((), ())), preferred_element_type=F32)


def hot(rows, index):
    ids = lax.broadcasted_iota(jnp.int32, (rows, index.shape[1]), 0)
    return jnp.where(ids == index, 1.0, 0.0).astype(BF)


PLAN = (
    ("first", 1), ("first", 4), ("mark", None), ("first", 0), ("second", 1), ("collect", None), ("second", 4),
    ("turn", 1), ("second", 0), ("first", 2), ("turn", 0), ("direct", 1), ("last", 1), ("direct", 0),
    ("second", 2), ("lift1", 1), ("links", None), ("turn", 2), ("last", 0), ("lift2", 1), ("lift3", 1),
    ("first", 3), ("arrive", 0), ("turn", 4), ("embed", None), ("direct", 2), ("arrive", 1), ("first", 5),
    ("second", 3), ("encode", None), ("ring", None), ("last", 2), ("turn", 3), ("direct", 4), ("arrive", 2),
    ("lift1", 4), ("last", 4), ("project", None), ("turn", 5), ("second", 5), ("near0", None),
    ("near1", None), ("direct", 3), ("last", 3), ("lift2", 4), ("outer", None), ("far1", None), ("lift3", 4),
    ("direct", 5), ("last", 5), ("far0", None), ("arrive", 3), ("gather", None), ("arrive", 4),
    ("node", None),
)


def kernel(
    n_face, n_sub,
    mesh_hbm, edge_hbm, grid_hbm, send_hbm, recv_hbm, lists_hbm, src_hbm, dst_hbm, area_hbm,
    wg, we, w1, w2, v1, v2,
    lat_out, edges, mass_out,
    gg, ge, g1, g2, h1, h2,
    mesh_ref, grid_ref, send_ref, recv_ref, lists_ref, src_ref, dst_ref, area_ref,
    picks, back, link_pick, table, proj, halo, parts, total, into, ahead, partial, hiddens, area_col,
    s1, r1, s2, r2, s3, r3, hs, hr, ms, mr, ein, win, pin,
):
    face, sub = lax.axis_index("face"), lax.axis_index("sub")
    core = lax.rem(face, 2)
    partner = face + 1 - 2 * core
    level = lax.rem(face // 2, 2)
    beside = face + 2 - 4 * level
    nodes, width = mesh_ref.shape
    chunks = edges.shape[0] // CHUNK
    size = halo.shape[1]
    slots = nodes + 4 * size

    load_edges = pltpu.make_async_copy(edge_hbm, edges, ein)

    shards = [wg, we, w1.at[0], w2.at[0], v1.at[0], v2.at[0]]
    wholes = [gg, ge, g1, g2, h1, h2]

    def rows_of(w, owner, start, count):
        rows = shards[w].shape[0]
        return wholes[w].at[pl.ds(pl.multiple_of(owner * rows + start, count), count)]

    def own(w):
        return pltpu.make_async_copy(shards[w], rows_of(w, sub, 0, shards[w].shape[0]), win.at[w])

    pairs = [(send_hbm, send_ref), (recv_hbm, recv_ref), (src_hbm, src_ref), (dst_hbm, dst_ref),
             (grid_hbm, grid_ref), (mesh_hbm, mesh_ref), (lists_hbm, lists_ref), (area_hbm, area_ref)]
    loads = [pltpu.make_async_copy(a, b, pin.at[i]) for i, (a, b) in enumerate(pairs)]
    for w in (1, 0, 4):
        own(w).start()
    for copy in loads:
        copy.start()
    for w in (2, 3, 5):
        own(w).start()
    load_edges.start()

    others = [(lax.rem(face + a, n_face), lax.rem(sub + b, n_sub))
              for a in range(n_face) for b in range(n_sub) if a or b]
    barrier = pltpu.get_barrier_semaphore()
    for peer in others:
        pl.semaphore_signal(barrier, inc=1, device_id=peer, device_id_type=MESH)
    pl.semaphore_wait(barrier, len(others))

    bits = [1 << b for b in range(n_sub.bit_length() - 1)]
    orders = (bits, bits[::-1])
    masks = range(1, n_sub)

    def across_bits(mask):
        index = sub
        for bit in bits:
            if mask & bit:
                index = index + bit - 2 * bit * lax.rem(index // bit, 2)
        return index

    def top(path, mask):
        return max(t for t, bit in enumerate(orders[path]) if mask & bit)

    def piece(w, path, mask, other_level=False):
        rows = shards[w].shape[0]
        if w in LEVELLED:
            count = rows // 8
            at = 1 - level if other_level else level
            start = (core * 4 + at * 2 + path) * count
        else:
            count = rows // 4
            start = (core * 2 + path) * count
        return rows_of(w, across_bits(mask), start, count)

    final = len(bits) - 1
    groups = [[(p, m) for m in masks for p in (0, 1) if top(p, m) == t] for t in range(final)]
    groups.append([(p, m) for p in (0, 1) for m in bits if top(p, m) == final])
    groups.append([(p, m) for m in masks for p in (0, 1) if top(p, m) == final and m not in bits])
    turns, direct, last = range(final), (final,), (final + 1,)
    group_of = {pm: g for g, group in enumerate(groups) for pm in group}

    def settle(w, count, sem):
        rows = wholes[w].at[pl.ds(0, count)]
        pltpu.make_async_copy(rows, rows, sem).wait()

    def cut(w):
        return shards[w].shape[0] // (8 if w in LEVELLED else 4)

    def outward(w, path, mask):
        bit = orders[path][top(path, mask)]
        part = piece(w, path, mask - bit)
        return pltpu.make_async_remote_copy(
            src_ref=part, dst_ref=part, send_sem=s1.at[w], recv_sem=r1.at[w, group_of[path, mask]],
            device_id=(face, across_bits(bit)), device_id_type=MESH)

    def upward(w, path, mask):
        part = piece(w, path, mask)
        at = LEVELLED.index(w)
        return pltpu.make_async_remote_copy(
            src_ref=part, dst_ref=part, send_sem=s3.at[at], recv_sem=r3.at[at, group_of[path, mask]],
            device_id=(beside, sub), device_id_type=MESH)

    def across(w, path, mask, lifted):
        part = piece(w, path, mask, lifted)
        return pltpu.make_async_remote_copy(
            src_ref=part, dst_ref=part, send_sem=s2.at[w], recv_sem=r2.at[w],
            device_id=(partner, sub), device_id_type=MESH)

    def begin(w):
        own(w).wait()
        for p in (0, 1):
            outward(w, p, orders[p][0]).start()

    def rest(w):
        for p in (0, 1):
            for bit in orders[p][1:]:
                outward(w, p, bit).start()

    def take(which, w):
        for g in which:
            if not groups[g]:
                continue
            settle(w, len(groups[g]) * cut(w), r1.at[w, g])
            for p, m in groups[g]:
                for bit in orders[p][top(p, m) + 1:]:
                    outward(w, p, m + bit).start()
                if w in LEVELLED:
                    upward(w, p, m).start()
                across(w, p, m, False).start()

    def lift(which, w):
        for g in which:
            if not groups[g]:
                continue
            settle(w, len(groups[g]) * cut(w), r3.at[LEVELLED.index(w), g])
            for p, m in groups[g]:
                across(w, p, m, True).start()

    def arrive(w):
        settle(w, (n_sub - 1) * shards[w].shape[0] // 2, r2.at[w])

    def border(d):
        step = (1, n_face - 1, 1, n_sub - 1)[d]
        to = (lax.rem(face + step, n_face), sub) if d < 2 else (face, lax.rem(sub + step, n_sub))
        return pltpu.make_async_remote_copy(
            src_ref=halo.at[d], dst_ref=halo.at[4 + d], send_sem=hs, recv_sem=hr,
            device_id=to, device_id_type=MESH)

    def ready():
        while loads:
            loads.pop().wait()

    def mark():
        ready()

        def step(i, carry):
            cols = pl.ds(pl.multiple_of(i * CHUNK, CHUNK), CHUNK)
            here = hot(nodes, recv_ref[:, cols])
            back[:, cols] = here
            from_own = hot(nodes, send_ref[:, cols])
            from_other = hot(slots - nodes, send_ref[:, cols] - nodes)
            picks[cols, :] = jnp.concatenate([from_own, here, from_other], axis=0).T
            return carry

        lax.fori_loop(0, chunks, step, 0)

    def collect():
        load_edges.wait()
        total[...] = mm(back[...], edges[...])
        into[...] = jnp.zeros_like(into)
        area_col[...] = jnp.broadcast_to(area_ref[...], (LANES, nodes)).T

    grids = grid_ref.shape[0]

    def links():
        ready()
        link_pick[:grids, :] = hot(grids, src_ref[...])
        link_pick[grids:, :] = hot(nodes, dst_ref[...])

    def embed():
        depth = grid_ref.shape[1]
        grid = jnp.concatenate([mm(grid_ref[...], gg[j * depth:(j + 1) * depth, :]) for j in range(n_sub)], axis=1)
        table[...] = silu(grid).astype(BF)

    def encode():
        from_grid = mm(table[...], ge[:width, :]).astype(BF)
        from_mesh = mm(mesh_ref[...], ge[width:, :]).astype(BF)
        both = jnp.concatenate([from_grid, from_mesh], axis=0)
        message = silu(mm_t(link_pick[...], both)).astype(BF)
        table[...] = (mesh_ref[...].astype(F32) + mm(link_pick[grids:, :], message)).astype(BF)

    def ring():
        for d in range(4):
            halo[d] = mm_t(hot(nodes, lists_ref[0, d:d + 1, :]), table[...]).astype(BF)
        for d in range(4):
            border(d).start()

    def project():
        proj[:nodes, :] = mm(table[...], g1[width:2 * width, :]).astype(BF)
        proj[nodes:2 * nodes, :] = mm(table[...], g1[2 * width:, :]).astype(BF)

    def outer():
        lists = halo.at[pl.ds(0, 4)]
        pltpu.make_async_copy(lists, lists, hr).wait()
        rows = jnp.concatenate([halo[4 + d] for d in range(4)], axis=0)
        proj[2 * nodes:, :] = mm(rows, g1[width:2 * width, :]).astype(BF)

    def near(i):
        rows = slice(i * CHUNK, (i + 1) * CHUNK)
        partial[rows, :] = mm(edges[rows, :], g1[:width, :]) + mm(picks[rows, :2 * nodes], proj[:2 * nodes, :])

    def far(i):
        rows = slice(i * CHUNK, (i + 1) * CHUNK)
        before = partial[rows, :] + mm(picks[rows, 2 * nodes:], proj[2 * nodes:, :])
        hidden = silu(before).astype(BF)
        hiddens[rows, :] = hidden
        into[...] += mm(back[:, rows], hidden)

    def begin_node():
        ahead[...] = mm(table[...], h1[:width, :])

    def gather():
        high = into[...].astype(BF)
        low = (into[...] - high.astype(F32)).astype(BF)
        total[...] += mm(high, g2[...]) + mm(low, g2[...])

    steps = {
        "first": begin, "second": rest, "arrive": arrive,
        "turn": functools.partial(take, turns), "direct": functools.partial(take, direct),
        "last": functools.partial(take, last), "lift1": functools.partial(lift, turns),
        "lift2": functools.partial(lift, direct), "lift3": functools.partial(lift, last),
    }
    works = {"mark": mark, "collect": collect, "links": links, "embed": embed, "encode": encode, "ring": ring,
             "project": project, "outer": outer, "gather": gather, "node": begin_node}
    for i in range(chunks):
        works[f"near{i}"] = functools.partial(near, i)
        works[f"far{i}"] = functools.partial(far, i)
    for name, w in PLAN:
        if w is None:
            works[name]()
        else:
            steps[name](w)

    incoming = total[...].astype(BF)
    hidden = silu(ahead[...] + mm(incoming, h1[width:, :])).astype(BF)
    arrive(5)
    latest = (table[...].astype(F32) + mm(hidden, h2[...])).astype(BF)
    lat_out[...] = latest
    weight = jnp.concatenate([area_col[...]] * (width // LANES), axis=1)
    me = face * n_sub + sub
    parts[me] = jnp.sum(latest.astype(F32) * weight, axis=0, keepdims=True)

    def share(k):
        return pltpu.make_async_remote_copy(
            src_ref=parts.at[me], dst_ref=parts.at[me], send_sem=ms, recv_sem=mr,
            device_id=others[k], device_id_type=MESH)

    for k in range(len(others)):
        share(k).start()

    def update(i, carry):
        cols = pl.ds(pl.multiple_of(i * CHUNK, CHUNK), CHUNK)
        edges[cols, :] = (edges[cols, :].astype(F32) + mm(hiddens[cols, :], g2[...])).astype(BF)
        return carry

    lax.fori_loop(0, chunks, update, 0)
    heard = parts.at[pl.ds(0, len(others))]
    pltpu.make_async_copy(heard, heard, mr).wait()
    mass_out[...] = jnp.sum(parts[...], axis=0) / (nodes * n_face * n_sub)

    for w in range(6):
        settle(w, 2 * (n_sub - 1) * cut(w), s1.at[w])
        settle(w, (n_sub - 1) * shards[w].shape[0] // 2, s2.at[w])
        if w in LEVELLED:
            settle(w, 2 * (n_sub - 1) * cut(w), s3.at[LEVELLED.index(w)])
    pltpu.make_async_copy(halo.at[pl.ds(0, 4)], halo.at[pl.ds(0, 4)], hs).wait()
    pltpu.make_async_copy(heard, heard, ms).wait()


def put(lat, edges, mass, lat_out, edges_out, mass_out, sems):
    pairs = [(edges, edges_out), (lat, lat_out), (mass, mass_out)]
    copies = [pltpu.make_async_copy(a, b, sems.at[i]) for i, (a, b) in enumerate(pairs)]
    for copy in copies:
        copy.start()
    for copy in copies:
        copy.wait()


def per_device(
    mesh_latent, edge_latent, grid_features, senders, receivers, send_lists, link_sources,
    link_targets, node_area, grid_weight, encode_weight, edge_first, edge_second, node_first,
    node_second,
):
    n_face, n_sub = lax.axis_size("face"), lax.axis_size("sub")
    nodes, width = mesh_latent.shape
    count = edge_latent.shape[0]
    size = send_lists.shape[2]
    slots = nodes + 4 * size
    chunks = count // CHUNK
    dma = pltpu.SemaphoreType.DMA
    turns = n_sub.bit_length()
    vmem = pl.BlockSpec(memory_space=pltpu.VMEM)
    hbm = pl.BlockSpec(memory_space=pltpu.HBM)
    anywhere = pl.BlockSpec(memory_space=pl.ANY)
    whole = [pltpu.VMEM((n_sub * w.shape[-2], width), BF)
             for w in (encode_weight, edge_first, edge_second, node_first, node_second)]
    results = pl.pallas_call(
        functools.partial(kernel, n_face, n_sub),
        out_shape=(
            pltpu.VMEM(mesh_latent.shape, BF),
            pltpu.VMEM(edge_latent.shape, BF),
            pltpu.VMEM((1, width), F32),
        ),
        in_specs=[hbm] * 15,
        out_specs=(vmem, vmem, vmem),
        scratch_shapes=[
            pltpu.VMEM((n_sub * grid_weight.shape[0], grid_weight.shape[1]), BF), *whole,
            pltpu.VMEM(mesh_latent.shape, BF), pltpu.VMEM(grid_features.shape, BF),
            pltpu.VMEM((1, count), jnp.int32), pltpu.VMEM((1, count), jnp.int32),
            pltpu.VMEM(send_lists.shape, jnp.int32),
            pltpu.VMEM((1, link_sources.shape[0]), jnp.int32),
            pltpu.VMEM((1, link_targets.shape[0]), jnp.int32),
            pltpu.VMEM((1, nodes), F32),
            pltpu.VMEM((count, slots + nodes), BF),
            pltpu.VMEM((nodes, count), BF),
            pltpu.VMEM((grid_features.shape[0] + nodes, link_sources.shape[0]), BF),
            pltpu.VMEM((nodes, width), BF),
            pltpu.VMEM((slots + nodes, width), BF),
            pltpu.VMEM((8, size, width), BF),
            pltpu.VMEM((n_face * n_sub, 1, width), F32),
            pltpu.VMEM((nodes, width), F32),
            pltpu.VMEM((nodes, width), F32),
            pltpu.VMEM((nodes, width), F32),
            pltpu.VMEM(edge_latent.shape, F32),
            pltpu.VMEM(edge_latent.shape, BF),
            pltpu.VMEM((nodes, LANES), F32),
            dma((6,)), dma((6, turns)), dma((6,)), dma((6,)), dma((len(LEVELLED),)), dma((len(LEVELLED), turns)),
            *[dma(())] * 5, dma((6,)), dma((8,)),
        ],
        compiler_params=pltpu.CompilerParams(
            collective_id=0, has_side_effects=True, vmem_limit_bytes=62000000
        ),
    )(
        mesh_latent, edge_latent, grid_features, senders.reshape(1, -1), receivers.reshape(1, -1),
        send_lists, link_sources.reshape(1, -1), link_targets.reshape(1, -1),
        node_area.reshape(1, -1), grid_weight, encode_weight, edge_first, edge_second, node_first,
        node_second,
    )
    return pl.pallas_call(
        put,
        out_shape=tuple(jax.ShapeDtypeStruct(r.shape, r.dtype) for r in results),
        in_specs=[anywhere] * 3,
        out_specs=(anywhere,) * 3,
        scratch_shapes=[dma((3,))],
        compiler_params=pltpu.CompilerParams(vmem_limit_bytes=1 << 20),
    )(*results)


def solution(mesh):
    both = P(("face", "sub"))
    in_specs = (both,) * 9 + (P(None, "sub"), P("sub", None)) + (P(None, "sub", None),) * 4
    return jax.shard_map(
        per_device, mesh=mesh, in_specs=in_specs, out_specs=(both, both, P()), check_vma=False
    )
```
